32 devices in a mesh: tok: 8 (over y, x, core), col: 4 (over z).
Axes of the slice: x: 2, y: 2, z: 4, core: 2. Of those that a mesh axis runs over, the one named last changes fastest.
Arguments:
- acts_a: bfloat16 [8192, 3584], P('tok', 'col'), may hold values from -6 to 6
- acts_b: bfloat16 [8192, 4096], P('tok', 'col'), may hold values from -6 to 6
- whiten_a: bfloat16 [3584, 3584], P(None, 'col'), may hold values from -0.09375 to 0.09375
- whiten_b: bfloat16 [4096, 4096], P(None, 'col'), may hold values from -0.09375 to 0.09375
Outputs:
- cross: float32 [3584, 4096], P('col', 'tok')
The draws below stay inside these ranges and needn't reach their ends.
All inputs are finite; a program needn't handle non-finite values.
Results may differ from the reference program's by a relative error of at most 0.0041.
Values may be sent and summed in bfloat16 or wider, within the bound.
A program may use at most 128 MiB of HBM per device.

```python
import jax
import jax.numpy as jnp
from jax import lax

DA = 3584
DB = 4096
TOKENS = 8192


def shard_levels(own_key, shape, pieces, low, top_value):
    def one(dim, shards_of):
        heights = jax.random.uniform(jax.random.fold_in(jax.random.fold_in(own_key, 6), dim), (shards_of,), jnp.float32, low / len(pieces), top_value / len(pieces))
        return jnp.repeat(jnp.exp(heights), shape[dim] // shards_of).reshape((-1,) + (1,) * (len(shape) - dim - 1))

    loudness = one(*pieces[0])
    for cut in pieces[1:]:
        loudness = loudness * one(*cut)
    return loudness


def bell_draw(key, shape, spread, bound, shards=(), held_as=jnp.bfloat16):
    drawn = jax.random.normal(key, shape, jnp.float32) * spread
    if len(shards) > 0:
        drawn = shard_levels(key, shape, shards, -0.22, 0.18) * drawn
    return jnp.clip(drawn, min=-bound, max=bound).astype(held_as)


def setup_inputs(seed: int = 0) -> dict:
    streams_of = jax.random.split(jax.random.key(seed), 5)
    acts_a = bell_draw(streams_of[0], (TOKENS, DA), 1.0, 6.0, ((0, 8), (1, 4)))
    acts_b = bell_draw(streams_of[1], (TOKENS, DB), 1.0, 6.0, ((0, 8), (1, 4)))
    whiten_a = bell_draw(streams_of[2], (DA, DA), DA ** -0.5, 0.09375, ((1, 4),))
    whiten_b = bell_draw(streams_of[3], (DB, DB), DB ** -0.5, 0.09375, ((1, 4),))
    return {"acts_a": acts_a, "acts_b": acts_b, "whiten_a": whiten_a, "whiten_b": whiten_b}


def reference(acts_a, acts_b, whiten_a, whiten_b):
    white_a = jnp.dot(acts_a, whiten_a, preferred_element_type=jnp.float32).astype(jnp.bfloat16)
    white_b = jnp.dot(acts_b, whiten_b, preferred_element_type=jnp.float32).astype(jnp.bfloat16)
    summed = lax.dot_general(white_a, white_b, (((0,), (0,)), ((), ())), preferred_element_type=jnp.float32)
    scale = 1.0 / jnp.sqrt(jnp.float32(TOKENS))
    return summed * scale
```

```python
import jax
import jax.numpy as jnp
from jax import lax
from jax.sharding import PartitionSpec as P

LANES = 128
SHARES = (5, 2)


def dot_tn(x, y):
    return lax.dot_general(x, y, (((0,), (0,)), ((), ())), preferred_element_type=jnp.float32)


def swap(x, step):
    return lax.ppermute(x, "tok", [(i, i ^ step) for i in range(lax.axis_size("tok"))])


def sum_tokens(part):
    size = lax.axis_size("tok")
    count = size.bit_length() - 1
    me = lax.axis_index("tok")
    rows, cols = part.shape
    done = []
    for flip in range(2):
        half = part[:, flip * (cols // 2):(flip + 1) * (cols // 2)]
        half = half.reshape((2,) * count + (rows // size, cols // 2))
        left = list(range(count - 1, -1, -1))
        for bit in [0] + list(range(1, count))[:: -1 if flip else 1]:
            axis = left.index(bit)
            mine = (me >> bit) & 1
            keep = lax.dynamic_index_in_dim(half, mine, axis, keepdims=False)
            send = lax.dynamic_index_in_dim(half, 1 - mine, axis, keepdims=False)
            half = keep + swap(send, 1 << bit)
            left.remove(bit)
        done.append(half.astype(jnp.bfloat16))
    return jnp.concatenate(done, axis=1)


def line_gather(x):
    n = lax.axis_size("col")
    z = lax.axis_index("col")
    rows, w = x.shape
    ups, downs = [x], [x]
    for s in range(1, n):
        ups.append(lax.ppermute(ups[-1], "col", [(i, i + 1) for i in range(s - 1, n - 1)]))
        downs.append(lax.ppermute(downs[-1], "col", [(i, i - 1) for i in range(1, n - s + 1)]))
    out = lax.dynamic_update_slice_in_dim(jnp.zeros((rows, n * w), x.dtype), x, z * w, 1)
    for s in range(1, n):
        block = jnp.where(z >= s, ups[s], downs[n - s])
        out = lax.dynamic_update_slice_in_dim(out, block, ((z + n - s) % n) * w, 1)
    return out


def chunks(width):
    if width % (LANES * sum(SHARES)):
        return [(0, width)]
    unit, at, out = width // sum(SHARES), 0, []
    for share in SHARES:
        out.append((at, share * unit))
        at += share * unit
    return out


def body(acts_a, acts_b, whiten_a, whiten_b):
    n, m = lax.axis_size("col"), lax.axis_size("tok")
    tokens, width = acts_a.shape

    parts = chunks(width)
    gathered = [lax.all_gather(acts_a[:, at:at + w], "col", axis=1, tiled=True) for at, w in parts]
    covs, right = [], acts_b
    for g in gathered:
        cov = sum_tokens(dot_tn(g, right))
        cov, right = lax.optimization_barrier((cov, right))
        covs.append(cov)
    covs = [line_gather(c) for c in covs]
    whiten_b, _ = lax.optimization_barrier((whiten_b, cov))
    halves = [jnp.dot(c, whiten_b, preferred_element_type=jnp.float32).astype(jnp.bfloat16) for c in covs]
    halves = [lax.all_gather(h, "col", axis=1, tiled=True) for h in halves]

    total = None
    for (at, w), half in zip(parts, halves):
        half = lax.all_to_all(half, "tok", split_axis=1, concat_axis=0, tiled=True)
        weights = whiten_a.reshape(n, width, -1)[:, at:at + w].reshape(n * w, -1)
        term = dot_tn(weights, half)
        total = term if total is None else total + term
    scale = 1.0 / jnp.sqrt(jnp.float32(tokens * m))
    return total * scale


def solution(mesh):
    placed = (P("tok", "col"), P("tok", "col"), P(None, "col"), P(None, "col"))
    return jax.shard_map(
        body, mesh=mesh, in_specs=placed, out_specs=P("col", "tok"), check_vma=False
    )
```
